32 devices in a mesh: outer: 4 (over y, x), inner: 8 (over z, core).
Axes of the slice: x: 2, y: 2, z: 4, core: 2. Of those that a mesh axis runs over, the one named last changes fastest.
Arguments:
- acts: bfloat16 [32, 2, 512, 512], P(('outer', 'inner')), may hold values from -6 to 6
- cotangent: bfloat16 [32, 2, 512, 512], P(('outer', 'inner')), may hold values from -6 to 6
- residual: float32 [32, 2048, 128], P(('outer', 'inner')), may hold values from -0.6 to 0.6
- owner_residual: float32 [32, 256, 128], P(('outer', 'inner')), may hold values from -3 to 3
- in_count: int32 [32, 2, 8], P(('outer', 'inner')), may hold values from 1 to 128, as said below
- in_rank: int32 [32, 2, 2048], P(('outer', 'inner')), may hold values from 0 to 255, as said below
- out_count: int32 [32, 2], P(('outer', 'inner')), may hold values from 1 to 128
- out_rank: int32 [32, 2, 256], P(('outer', 'inner')), may hold values from 0 to 255, as said below
Outputs:
- applied: bfloat16 [512, 512], replicated
- new_residual: float32 [32, 2048, 128], P(('outer', 'inner'))
- new_owner_residual: float32 [32, 256, 128], P(('outer', 'inner'))
The draws below stay inside these ranges and needn't reach their ends.
Inputs may be any that keep to these rules, and one draw needn't show every extreme that they name: `in_count`: each step has one owner that receives 128 blocks from every replica. `in_rank`: for each replica, step and owner, the ranks of that owner's 256 blocks are a permutation of 0 to 255. `out_rank`: for each replica and step a permutation of 0 to 255.
All inputs are finite; a program needn't handle non-finite values.
Results may differ from the reference program's by a relative error of at most 0.0065.
Values may be sent and summed in bfloat16 or wider, within the bound.
A program may use at most 64 MiB of HBM per device.

```python
import math
import jax
import jax.numpy as jnp
from jax import lax

TILE_R = 512
TILE_C = 512
BLOCK = 128
STEPS = 2
TOK = 512
REPLICAS = 32
BLOCKS = 2048
REGION = 256
CAP = 128
N_OUTER = 4
N_INNER = 8


def skewed_counts(key, shape):
    first = jax.random.randint(jax.random.fold_in(key, 1), shape, 0, CAP)
    second = jax.random.randint(jax.random.fold_in(key, 2), shape, 0, CAP)
    return jnp.minimum(first, second) + 1


def draw_in_count(key, part):
    counts = skewed_counts(jax.random.fold_in(key, 11), (REPLICAS, STEPS, N_INNER))
    hottest = jax.random.randint(jax.random.fold_in(key, 5), (STEPS,), 0, N_INNER)
    owners = jnp.arange(N_INNER)[None, None, :]
    return jnp.where(owners == hottest[None, :, None], CAP, counts).astype(jnp.int32)


def permutations(key, count):
    keys = jax.random.split(key, count)
    return jax.vmap(lambda single: jax.random.permutation(single, REGION))(keys)


def draw_in_rank(key, part):
    ranks = permutations(jax.random.fold_in(key, 13), REPLICAS * STEPS * N_INNER)
    return ranks.reshape(REPLICAS, STEPS, BLOCKS).astype(jnp.int32)


def draw_out_count(key, part):
    counts = skewed_counts(jax.random.fold_in(key, 17), (REPLICAS, STEPS))
    fullest = jax.random.randint(jax.random.fold_in(key, 19), (STEPS,), 0, REPLICAS)
    rows = jnp.arange(REPLICAS)[:, None]
    return jnp.where(rows == fullest[None, :], CAP, counts).astype(jnp.int32)


def draw_out_rank(key, part):
    ranks = permutations(jax.random.fold_in(key, 23), REPLICAS * STEPS)
    return ranks.reshape(REPLICAS, STEPS, REGION).astype(jnp.int32)


def block_scale(key, shape, cuts, smallest, largest):
    factor_of, own = 1.0, jax.random.fold_in(key, 6)
    for axis_at, blocks in cuts:
        draws = jnp.exp(jax.random.uniform(jax.random.fold_in(own, axis_at), (blocks,), jnp.float32, smallest / len(cuts), largest / len(cuts)))
        factor_of = factor_of * jnp.repeat(draws, shape[axis_at] // blocks).reshape([-1 if axis == axis_at else 1 for axis in range(len(shape))])
    return factor_of


def normal_values(rng, shape, width, bound, cuts=(), kind=jnp.bfloat16):
    drawn = width * jax.random.normal(rng, shape, jnp.float32)
    if cuts:
        drawn = drawn * block_scale(rng, shape, cuts, -0.22, 0.18)
    return jnp.clip(drawn, -bound, bound).astype(kind)


def setup_inputs(seed: int = 0) -> dict:
    key_of = jax.random.split(jax.random.key(seed), 9)
    return {
        "acts": normal_values(key_of[0], (REPLICAS, STEPS, TOK, TILE_R), 1.0, 6.0, ((0, 32),)),
        "cotangent": normal_values(key_of[1], (REPLICAS, STEPS, TOK, TILE_C), 1.0, 6.0, ((0, 32),)),
        "residual": normal_values(key_of[2], (REPLICAS, BLOCKS, BLOCK), 0.1, 0.6, ((0, 32),), jnp.float32),
        "owner_residual": normal_values(key_of[3], (REPLICAS, REGION, BLOCK), 0.5, 3.0, ((0, 32),), jnp.float32),
        "in_count": draw_in_count(jax.random.fold_in(key_of[8], 71), 0),
        "in_rank": draw_in_rank(jax.random.fold_in(key_of[8], 71), 0),
        "out_count": draw_out_count(jax.random.fold_in(key_of[8], 71), 0),
        "out_rank": draw_out_rank(jax.random.fold_in(key_of[8], 71), 0),
    }


step_size = 0.0625

def local_grad(pair):
    left, right = pair
    return jnp.einsum('tr,tc->rc', left.astype(jnp.float32), right.astype(jnp.float32), precision=lax.Precision.HIGHEST)

def reference(acts, cotangent, residual, owner_residual, in_count, in_rank, out_count, out_rank):
    scale = 1.0 / math.sqrt(TOK * N_INNER)
    resid = residual
    oresid = owner_residual.reshape(N_OUTER, BLOCKS, BLOCK)
    total = jnp.zeros((BLOCKS, BLOCK), jnp.float32)
    for step in range(STEPS):
        grads = lax.map(local_grad, (acts[:, step], cotangent[:, step]))
        accum = resid + (grads * scale).reshape(REPLICAS, BLOCKS, BLOCK)
        counts = jnp.repeat(in_count[:, step], REGION, axis=1)
        chosen = (in_rank[:, step] < counts)[..., None]
        sent = jnp.where(chosen, accum, jnp.float32(0.0))
        resid = jnp.where(chosen, jnp.float32(0.0), accum)
        pod_sum = lax.optimization_barrier(jnp.sum(sent.reshape(N_OUTER, N_INNER, BLOCKS, BLOCK), axis=1))
        owner_acc = pod_sum + oresid
        ocounts = jnp.repeat(out_count[:, step].reshape(N_OUTER, N_INNER), REGION, axis=1)
        passed = (out_rank[:, step].reshape(N_OUTER, BLOCKS) < ocounts)[..., None]
        cross = lax.optimization_barrier(jnp.sum(jnp.where(passed, owner_acc, jnp.float32(0.0)), axis=0))
        oresid = jnp.where(passed, jnp.float32(0.0), owner_acc)
        delta = cross.astype(jnp.bfloat16)
        total = total + delta.astype(jnp.float32)
    applied = (-step_size * total).astype(jnp.bfloat16).reshape(TILE_R, TILE_C)
    return (applied, resid, oresid.reshape(REPLICAS, REGION, BLOCK))
```

```python
import functools
import math

import jax
import jax.numpy as jnp
from jax import lax
from jax.experimental import pallas as pl
from jax.experimental.pallas import tpu as pltpu
from jax.sharding import PartitionSpec as P

step_size = 0.0625


def select_blocks(resid, grad, ranks_flat, counts, owners, region, width):
    blocks = resid.shape[0]
    accum = (resid + grad.reshape(blocks, width)).reshape(owners, region, width)
    ranks = ranks_flat.reshape(owners, region)
    chosen = (ranks < counts[:, None])[..., None]
    new_resid = jnp.where(chosen, jnp.float32(0.0), accum).reshape(blocks, width)
    return (accum, ranks, chosen, new_resid)


def pack_slots(accum, ranks, counts, slots, region):
    order = lax.iota(jnp.int32, slots)
    picks = (ranks[:, None, :] == order[None, :, None]) & (
        order[None, :, None] < counts[:, None, None]
    )
    picks_f = picks.astype(jnp.float32)
    places = lax.iota(jnp.int32, region).astype(jnp.float32)
    packed = jnp.einsum("nkr,nrd->nkd", picks_f, accum, precision=lax.Precision.HIGHEST)
    where_at = jnp.einsum("nkr,r->nk", picks_f, places, precision=lax.Precision.HIGHEST)
    return (packed, where_at)


def unpack_slots(arrived, spots, region, width):
    places = lax.iota(jnp.int32, region).astype(jnp.float32)
    placed = (spots.reshape(-1)[:, None] == places[None, :]).astype(jnp.float32)
    return jnp.einsum(
        "mr,md->rd", placed, arrived.reshape(-1, width), precision=lax.Precision.HIGHEST
    )


def owner_section(pod_sum, oresid, ranks_out, count_out):
    owner_acc = pod_sum + oresid
    passed = (ranks_out < count_out)[:, None]
    outgoing = jnp.where(passed, owner_acc, jnp.float32(0.0))
    kept = jnp.where(passed, jnp.float32(0.0), owner_acc)
    return (outgoing, kept)


def per_device(acts, cotangent, residual, owner_residual, in_count, in_rank, out_count, out_rank):
    owners = lax.axis_size("inner")
    steps = acts.shape[1]
    tokens = acts.shape[2]
    rows = acts.shape[3]
    cols = cotangent.shape[3]
    blocks = residual.shape[1]
    width = residual.shape[2]
    region = blocks // owners
    slots = max(1, region // 2)
    scale = 1.0 / math.sqrt(tokens * owners)
    resid = residual[0]
    oresid = owner_residual[0]
    crosses = []
    packs = []
    spots_all = []
    for step in range(steps):
        grad = (
            jnp.einsum(
                "tr,tc->rc", acts[0, step], cotangent[0, step], preferred_element_type=jnp.float32
            )
            * scale
        )
        counts = in_count[0, step]
        accum, ranks, chosen, resid = select_blocks(
            resid, grad, in_rank[0, step], counts, owners, region, width
        )
        packed, where_at = pack_slots(accum, ranks, counts, slots, region)
        packs.append(packed)
        spots_all.append(where_at)
    arrived, spots = (
        lax.all_to_all(
            jnp.concatenate(packs, axis=1), "inner", split_axis=0, concat_axis=0, tiled=True
        ),
        lax.all_to_all(
            jnp.concatenate(spots_all, axis=1), "inner", split_axis=0, concat_axis=0, tiled=True
        ),
    )
    outgoings = []
    for step in range(steps):
        pod_sum = unpack_slots(
            arrived[:, step * slots : (step + 1) * slots],
            spots[:, step * slots : (step + 1) * slots],
            region,
            width,
        )
        outgoing, oresid = owner_section(pod_sum, oresid, out_rank[0, step], out_count[0, step])
        outgoings.append(outgoing)
    summed = lax.psum(jnp.stack(outgoings), "outer")
    for step in range(steps):
        crosses.append(summed[step])
    deltas = []
    for cross in crosses:
        delta = cross.astype(jnp.bfloat16)
        deltas.append(lax.all_gather(delta, "inner", axis=0, tiled=True))
    total = deltas[0].astype(jnp.float32)
    for later in deltas[1:]:
        total = total + later.astype(jnp.float32)
    applied = (-step_size * total).astype(jnp.bfloat16)
    return (applied.reshape(rows, cols), resid[None], oresid[None])


LANES = 128
F32 = jnp.float32
BF16 = jnp.bfloat16


def fused_kernel(
    dims,
    acts_hbm, cot_hbm, res_hbm, ores_ref, cnt_ref, rank_ref, ocnt_ref, orank_ref,
    applied_ref, resid_hbm, nores_ref,
    acts_v, cot_v, res_v, rk_ref, rp_ref, mt_ref, rsend, rrecv, rall_ref, oh_ref,
    send, recv, xsend, xrecv, ag,
    in_sem, out_sem, rs_sem, rr_sem, s_sem, r_sem, xs_sem, xr_sem,
    zs_sem, zr_sem, os_sem, or_sem, ps_sem, pr_sem,
):
    n_in, n_out, steps, scale, region, slots, width = dims
    rows, cols = acts_v.shape[2], cot_v.shape[2]
    cpr = cols // width
    rpr = region // cpr
    halves = region // LANES
    rpc = LANES // rpr
    n_z = n_in // 2
    big = float(region)
    me = lax.axis_index("inner")
    pod = lax.axis_index("outer")
    core = lax.rem(me, 2)
    z = lax.div(me, 2)
    partner = me + 1 - 2 * core

    def inner(d):
        return lax.rem(me + d, n_in)

    def outer(d):
        return lax.rem(pod + d, n_out)

    def remote(src, dst, ssem, rsem, **device):
        return pltpu.make_async_remote_copy(
            src_ref=src, dst_ref=dst, send_sem=ssem, recv_sem=rsem,
            device_id=device, device_id_type=pl.DeviceIdType.MESH,
        )

    loads = []
    for s in range(steps):
        pair = [
            pltpu.make_async_copy(acts_hbm.at[s], acts_v.at[s], in_sem.at[2 * s]),
            pltpu.make_async_copy(cot_hbm.at[s], cot_v.at[s], in_sem.at[2 * s + 1]),
        ]
        for copy in pair:
            copy.start()
        loads.append(pair)
        if s == 0:
            res_load = pltpu.make_async_copy(res_hbm, res_v, in_sem.at[2 * steps])
            res_load.start()

    barrier = pltpu.get_barrier_semaphore()
    for d in range(1, n_in):
        pl.semaphore_signal(barrier, inc=1, device_id={"inner": inner(d)}, device_id_type=pl.DeviceIdType.MESH)
    for d in range(1, n_out):
        pl.semaphore_signal(barrier, inc=1, device_id={"outer": outer(d)}, device_id_type=pl.DeviceIdType.MESH)

    rk_ref[...] = jnp.full(rk_ref.shape, big, F32)
    for s in range(steps):
        for j in range(n_in):
            row = rank_ref[s : s + 1, j * region : (j + 1) * region]
            rk_ref[s * n_in + j : s * n_in + j + 1, :] = jnp.where(
                row < cnt_ref[s : s + 1, j : j + 1], row.astype(F32), big
            )
        row = orank_ref[s : s + 1, :]
        rk_ref[steps * n_in + s : steps * n_in + s + 1, :] = jnp.where(
            row < ocnt_ref[0:1, s : s + 1], row.astype(F32), big
        )
    old = lax.broadcasted_iota(jnp.int32, (region, region), 0)
    new = lax.broadcasted_iota(jnp.int32, (region, region), 1)
    shift = rpr.bit_length() - 1
    perm = jnp.where(old == (new & (rpr - 1)) * cpr + (new >> shift), 1.0, 0.0).astype(BF16)
    rp = jnp.dot(rk_ref[...].astype(BF16), perm, preferred_element_type=F32)
    rp_ref[...] = rp
    n_rk = rk_ref.shape[0]

    def eye(n):
        return jnp.where(
            lax.broadcasted_iota(jnp.int32, (n, LANES), 0) == lax.broadcasted_iota(jnp.int32, (n, LANES), 1), 1.0, 0.0
        ).astype(BF16)

    def turned(values):
        return lax.dot_general(
            values.astype(BF16), eye(values.shape[0]), (((0,), (0,)), ((), ())), preferred_element_type=F32
        ).astype(BF16)

    def spread(table, index, n):
        pick = jnp.where(lax.broadcasted_iota(jnp.int32, (LANES, n), 0) == index, 1.0, 0.0).astype(BF16)
        return jnp.dot(table, pick, preferred_element_type=F32)

    mt_ref[...] = turned(jnp.where(rp < big, 1.0, 0.0))
    for j in range(n_in):
        for s in range(steps):
            for h in range(halves):
                rsend[j, s * halves + h : s * halves + h + 1, :] = rp_ref[
                    s * n_in + j : s * n_in + j + 1, h * LANES : (h + 1) * LANES
                ]
    pl.semaphore_wait(barrier, n_in - 1 + n_out - 1)
    sends = []
    for d in range(1, n_in):
        copy = remote(rsend.at[inner(d)], rrecv.at[me], rs_sem.at[d], rr_sem.at[me], inner=inner(d))
        copy.start()
        sends.append(copy)

    order = []
    chunks = rows // LANES
    for a in range((chunks + 1) // 2):
        order.append(a)
        if chunks - 1 - a != a:
            order.append(chunks - 1 - a)

    def packet(s, j):
        return remote(send.at[s, j], recv.at[s, pl.ds(pl.multiple_of(me * slots, slots), slots)],
                      s_sem.at[s, j], r_sem.at[s, me], inner=j)

    slot_id = lax.broadcasted_iota(jnp.int32, (slots, region), 0).astype(F32)
    for s in range(steps):
        for copy in loads[s]:
            copy.wait()
        if s == 0:
            res_load.wait()
        for q in order:
            g = lax.dot_general(
                acts_v[s, :, q * LANES : (q + 1) * LANES], cot_v[s], (((0,), (0,)), ((), ())),
                preferred_element_type=F32,
            ) * scale
            for half in range(rpc):
                j = q * rpc + half
                chosen = spread(mt_ref[...], s * n_in + j, width)
                picks = jnp.where(rp_ref[s * n_in + j : s * n_in + j + 1, :] == slot_id, 1.0, 0.0).astype(BF16)
                parts = []
                for c in range(cpr):
                    where_at = pl.ds(region * j + c, rpr, stride=cpr)
                    acc = res_v[where_at, :] + g[half * rpr : (half + 1) * rpr, c * width : (c + 1) * width]
                    res_v[where_at, :] = jnp.where(chosen[c * rpr : (c + 1) * rpr] > 0.5, 0.0, acc)
                    parts.append(acc)
                packed = jnp.dot(picks, jnp.concatenate(parts, axis=0).astype(BF16), preferred_element_type=F32)
                send[s, j] = packed.astype(BF16)

                @pl.when(me != j)
                def _():
                    packet(s, j).start()

    resid_out = pltpu.make_async_copy(res_v, resid_hbm, out_sem)
    resid_out.start()

    rrecv[me] = rsend[me]
    for d in range(1, n_in):
        i = inner(d)
        remote(rrecv.at[i], rrecv.at[i], rs_sem.at[d], rr_sem.at[i], inner=i).wait_recv()
    for i in range(n_in):
        for s in range(steps):
            for h in range(halves):
                rall_ref[s * n_in + i : s * n_in + i + 1, h * LANES : (h + 1) * LANES] = rrecv[
                    i, s * halves + h : s * halves + h + 1, :
                ]
    rt = turned(rall_ref[...])
    lane_id = lax.broadcasted_iota(jnp.int32, (region, slots), 1).astype(F32)
    for s in range(steps):
        for i in range(n_in):
            oh_ref[s, :, i * slots : (i + 1) * slots] = jnp.where(
                spread(rt, s * n_in + i, slots) == lane_id, 1.0, 0.0
            ).astype(BF16)

    oresid = jnp.concatenate([ores_ref[pl.ds(c, rpr, stride=cpr), :] for c in range(cpr)], axis=0)
    for s in range(steps):
        recv[s, pl.ds(pl.multiple_of(me * slots, slots), slots)] = send[s, me]
        for d in range(1, n_in):
            i = inner(d)
            spot = recv.at[s, pl.ds(pl.multiple_of(i * slots, slots), slots)]
            remote(spot, spot, s_sem.at[s, 0], r_sem.at[s, i], inner=i).wait_recv()
        oacc = jnp.dot(oh_ref[s], recv[s], preferred_element_type=F32) + oresid
        passed = spread(mt_ref[...], steps * n_in + s, width) > 0.5
        outgoing = jnp.where(passed, oacc, 0.0).astype(BF16)
        oresid = jnp.where(passed, 0.0, oacc)
        for c in range(n_out):
            xsend[s, c] = outgoing[c * rpr : (c + 1) * rpr]
        for d in range(1, n_out):
            copy = remote(xsend.at[s, outer(d)], xrecv.at[s, pod], xs_sem.at[s, d], xr_sem.at[s, pod], outer=outer(d))
            copy.start()
            sends.append(copy)
    for c in range(cpr):
        nores_ref[pl.ds(c, rpr, stride=cpr), :] = oresid[c * rpr : (c + 1) * rpr]

    total = jnp.zeros((rpr, width), F32)
    for s in range(steps):
        cross = xsend[s, pod].astype(F32)
        for d in range(1, n_out):
            i = outer(d)
            remote(xrecv.at[s, i], xrecv.at[s, i], xs_sem.at[s, d], xr_sem.at[s, i], outer=i).wait_recv()
            cross = cross + xrecv[s, i].astype(F32)
        total = total + cross.astype(BF16).astype(F32)
    ag[core, pod, z] = (-step_size * total).astype(BF16)

    def forward(zz, slot):
        piece = ag.at[core, pod, zz]
        for d in range(1, n_out):
            copy = remote(piece, piece, os_sem.at[slot, d], or_sem.at[pod, zz], outer=outer(d))
            copy.start()
            sends.append(copy)

    def hand_over(q, slot):
        piece = ag.at[core, q]
        copy = remote(piece, piece, ps_sem.at[slot], pr_sem.at[q], inner=partner)
        copy.start()
        sends.append(copy)

    own = ag.at[core, pod, z]
    for d in range(1, n_z):
        copy = remote(own, own, zs_sem.at[d], zr_sem.at[z], inner=inner(2 * d))
        copy.start()
        sends.append(copy)
    forward(z, 0)
    for d in range(1, n_z):
        zz = lax.rem(z + d, n_z)
        piece = ag.at[core, pod, zz]
        remote(piece, piece, zs_sem.at[d], zr_sem.at[zz], inner=inner(2 * d)).wait_recv()
        forward(zz, d)
    hand_over(pod, 0)
    for d in range(1, n_out):
        q = outer(d)
        for zz in range(n_z):
            piece = ag.at[core, q, zz]
            remote(piece, piece, os_sem.at[0, d], or_sem.at[q, zz], outer=q).wait_recv()
        hand_over(q, d)
    for d in range(n_out):
        q = outer(d)
        piece = ag.at[1 - core, q]
        remote(piece, piece, ps_sem.at[d], pr_sem.at[q], inner=partner).wait_recv()
    for zz in range(n_z):
        for k in range(2):
            j = zz * 2 + k
            for q in range(n_out):
                applied_ref[j * rpr : (j + 1) * rpr, q * width : (q + 1) * width] = ag[k, q, zz]

    for copy in sends:
        copy.wait_send()
    for s in range(steps):
        for j in range(n_in):

            @pl.when(me != j)
            def _():
                packet(s, j).wait_send()

    resid_out.wait()


def fits(owners, pods, steps, rows, cols, blocks, width, region, slots):
    if width != LANES or slots % LANES or region % LANES or region > 256 or cols % width:
        return False
    cpr = cols // width
    rpr = region // cpr
    return (
        cpr == pods and cpr * rpr == region and rpr % 16 == 0 and LANES % rpr == 0 and rpr & (rpr - 1) == 0
        and rows % LANES == 0 and owners >= 4 and owners % 2 == 0
        and rpr * owners == rows and steps * (owners + 1) <= LANES and steps * (region // LANES) <= 8
    )


def per_device_fused(acts, cotangent, residual, owner_residual, in_count, in_rank, out_count, out_rank):
    n_in = lax.axis_size("inner")
    n_out = lax.axis_size("outer")
    steps, tokens, rows = acts.shape[1:]
    cols = cotangent.shape[3]
    blocks, width = residual.shape[1:]
    region = blocks // n_in
    slots = max(1, region // 2)
    if not fits(n_in, n_out, steps, rows, cols, blocks, width, region, slots):
        return per_device(acts, cotangent, residual, owner_residual, in_count, in_rank, out_count, out_rank)
    scale = 1.0 / math.sqrt(tokens * n_in)
    rpr = region // n_out
    n_z = n_in // 2
    n_rk = -(-steps * (n_in + 1) // 16) * 16
    n_ra = -(-steps * n_in // 16) * 16
    vmem = pl.BlockSpec(memory_space=pltpu.VMEM)
    anywhere = pl.BlockSpec(memory_space=pl.ANY)
    dma = pltpu.SemaphoreType.DMA
    applied, resid, oresid = pl.pallas_call(
        functools.partial(fused_kernel, (n_in, n_out, steps, scale, region, slots, width)),
        out_shape=(
            jax.ShapeDtypeStruct((rows, cols), BF16),
            jax.ShapeDtypeStruct((blocks, width), F32),
            jax.ShapeDtypeStruct((region, width), F32),
        ),
        in_specs=[anywhere, anywhere, anywhere, vmem, vmem, vmem, vmem, vmem],
        out_specs=(vmem, anywhere, vmem),
        scratch_shapes=[
            pltpu.VMEM((steps, tokens, rows), BF16),
            pltpu.VMEM((steps, tokens, cols), BF16),
            pltpu.VMEM((blocks, width), F32),
            pltpu.VMEM((n_rk, region), F32),
            pltpu.VMEM((n_rk, region), F32),
            pltpu.VMEM((region, LANES), BF16),
            pltpu.VMEM((n_in, 8, LANES), F32),
            pltpu.VMEM((n_in, 8, LANES), F32),
            pltpu.VMEM((n_ra, region), F32),
            pltpu.VMEM((steps, region, n_in * slots), BF16),
            pltpu.VMEM((steps, n_in, slots, width), BF16),
            pltpu.VMEM((steps, n_in * slots, width), BF16),
            pltpu.VMEM((steps, n_out, rpr, width), BF16),
            pltpu.VMEM((steps, n_out, rpr, width), BF16),
            pltpu.VMEM((2, n_out, n_z, rpr, width), BF16),
            dma((2 * steps + 1,)),
            dma,
            dma((n_in,)),
            dma((n_in,)),
            dma((steps, n_in)),
            dma((steps, n_in)),
            dma((steps, n_out)),
            dma((steps, n_out)),
            dma((n_z,)),
            dma((n_z,)),
            dma((n_z, n_out)),
            dma((n_out, n_z)),
            dma((n_out,)),
            dma((n_out,)),
        ],
        compiler_params=pltpu.CompilerParams(collective_id=0, has_side_effects=True),
    )(acts[0], cotangent[0], residual[0], owner_residual[0], in_count[0], in_rank[0], out_count, out_rank[0])
    return applied, resid[None], oresid[None]


def solution(mesh):
    return jax.shard_map(
        per_device_fused,
        mesh=mesh,
        in_specs=(
            P(("outer", "inner"), None, None, None),
            P(("outer", "inner"), None, None, None),
            P(("outer", "inner"), None, None),
            P(("outer", "inner"), None, None),
            P(("outer", "inner"), None, None),
            P(("outer", "inner"), None, None),
            P(("outer", "inner"), None),
            P(("outer", "inner"), None, None),
        ),
        out_specs=(P(), P(("outer", "inner"), None, None), P(("outer", "inner"), None, None)),
        check_vma=False,
    )
```

```python
import functools
import math

import jax
import jax.numpy as jnp
from jax import lax
from jax.experimental import pallas as pl
from jax.experimental.pallas import tpu as pltpu
from jax.sharding import PartitionSpec as P

step_size = 0.0625


def select_blocks(resid, grad, ranks_flat, counts, owners, region, width):
    blocks = resid.shape[0]
    accum = (resid + grad.reshape(blocks, width)).reshape(owners, region, width)
    ranks = ranks_flat.reshape(owners, region)
    chosen = (ranks < counts[:, None])[..., None]
    new_resid = jnp.where(chosen, jnp.float32(0.0), accum).reshape(blocks, width)
    return (accum, ranks, chosen, new_resid)


def pack_slots(accum, ranks, counts, slots, region):
    order = lax.iota(jnp.int32, slots)
    picks = (ranks[:, None, :] == order[None, :, None]) & (
        order[None, :, None] < counts[:, None, None]
    )
    picks_f = picks.astype(jnp.float32)
    places = lax.iota(jnp.int32, region).astype(jnp.float32)
    packed = jnp.einsum("nkr,nrd->nkd", picks_f, accum, precision=lax.Precision.HIGHEST)
    where_at = jnp.einsum("nkr,r->nk", picks_f, places, precision=lax.Precision.HIGHEST)
    return (packed, where_at)


def unpack_slots(arrived, spots, region, width):
    places = lax.iota(jnp.int32, region).astype(jnp.float32)
    placed = (spots.reshape(-1)[:, None] == places[None, :]).astype(jnp.float32)
    return jnp.einsum(
        "mr,md->rd", placed, arrived.reshape(-1, width), precision=lax.Precision.HIGHEST
    )


def owner_section(pod_sum, oresid, ranks_out, count_out):
    owner_acc = pod_sum + oresid
    passed = (ranks_out < count_out)[:, None]
    outgoing = jnp.where(passed, owner_acc, jnp.float32(0.0))
    kept = jnp.where(passed, jnp.float32(0.0), owner_acc)
    return (outgoing, kept)


def per_device(acts, cotangent, residual, owner_residual, in_count, in_rank, out_count, out_rank):
    owners = lax.axis_size("inner")
    steps = acts.shape[1]
    tokens = acts.shape[2]
    rows = acts.shape[3]
    cols = cotangent.shape[3]
    blocks = residual.shape[1]
    width = residual.shape[2]
    region = blocks // owners
    slots = max(1, region // 2)
    scale = 1.0 / math.sqrt(tokens * owners)
    resid = residual[0]
    oresid = owner_residual[0]
    crosses = []
    packs = []
    spots_all = []
    for step in range(steps):
        grad = (
            jnp.einsum(
                "tr,tc->rc", acts[0, step], cotangent[0, step], preferred_element_type=jnp.float32
            )
            * scale
        )
        counts = in_count[0, step]
        accum, ranks, chosen, resid = select_blocks(
            resid, grad, in_rank[0, step], counts, owners, region, width
        )
        packed, where_at = pack_slots(accum, ranks, counts, slots, region)
        packs.append(packed)
        spots_all.append(where_at)
    arrived, spots = (
        lax.all_to_all(
            jnp.concatenate(packs, axis=1), "inner", split_axis=0, concat_axis=0, tiled=True
        ),
        lax.all_to_all(
            jnp.concatenate(spots_all, axis=1), "inner", split_axis=0, concat_axis=0, tiled=True
        ),
    )
    outgoings = []
    for step in range(steps):
        pod_sum = unpack_slots(
            arrived[:, step * slots : (step + 1) * slots],
            spots[:, step * slots : (step + 1) * slots],
            region,
            width,
        )
        outgoing, oresid = owner_section(pod_sum, oresid, out_rank[0, step], out_count[0, step])
        outgoings.append(outgoing)
    summed = lax.psum(jnp.stack(outgoings), "outer")
    for step in range(steps):
        crosses.append(summed[step])
    deltas = []
    for cross in crosses:
        delta = cross.astype(jnp.bfloat16)
        deltas.append(lax.all_gather(delta, "inner", axis=0, tiled=True))
    total = deltas[0].astype(jnp.float32)
    for later in deltas[1:]:
        total = total + later.astype(jnp.float32)
    applied = (-step_size * total).astype(jnp.bfloat16)
    return (applied.reshape(rows, cols), resid[None], oresid[None])


LANES = 128
F32 = jnp.float32
BF16 = jnp.bfloat16


def fused_kernel(
    dims,
    acts_hbm, cot_hbm, res_hbm, ores_ref, cnt_ref, rank_ref, ocnt_ref, orank_ref,
    applied_ref, resid_ref, nores_ref,
    acts_v, cot_v, res_v, rk_ref, rp_ref, mt_ref, rsend, rrecv, rall_ref, oh_ref,
    send, recv, xsend, xrecv, ag,
    in_sem, rs_sem, rr_sem, s_sem, r_sem, xs_sem, xr_sem,
    zs_sem, zr_sem, os_sem, or_sem, ps_sem, pr_sem,
):
    n_in, n_out, steps, scale, region, slots, width = dims
    rows, cols = acts_v.shape[2], cot_v.shape[2]
    cpr = cols // width
    rpr = region // cpr
    halves = region // LANES
    rpc = LANES // rpr
    n_z = n_in // 2
    big = float(region)
    me = lax.axis_index("inner")
    pod = lax.axis_index("outer")
    core = lax.rem(me, 2)
    z = lax.div(me, 2)
    partner = me + 1 - 2 * core

    def inner(d):
        return lax.rem(me + d, n_in)

    def outer(d):
        return lax.rem(pod + d, n_out)

    def remote(src, dst, ssem, rsem, **device):
        return pltpu.make_async_remote_copy(
            src_ref=src, dst_ref=dst, send_sem=ssem, recv_sem=rsem,
            device_id=device, device_id_type=pl.DeviceIdType.MESH,
        )

    loads = []
    for s in range(steps):
        pair = [
            pltpu.make_async_copy(acts_hbm.at[s], acts_v.at[s], in_sem.at[2 * s]),
            pltpu.make_async_copy(cot_hbm.at[s], cot_v.at[s], in_sem.at[2 * s + 1]),
        ]
        for copy in pair:
            copy.start()
        loads.append(pair)
        if s == 0:
            res_load = pltpu.make_async_copy(res_hbm, res_v, in_sem.at[2 * steps])
            res_load.start()

    barrier = pltpu.get_barrier_semaphore()
    for d in range(1, n_in):
        pl.semaphore_signal(barrier, inc=1, device_id={"inner": inner(d)}, device_id_type=pl.DeviceIdType.MESH)
    for d in range(1, n_out):
        pl.semaphore_signal(barrier, inc=1, device_id={"outer": outer(d)}, device_id_type=pl.DeviceIdType.MESH)

    rk_ref[...] = jnp.full(rk_ref.shape, big, F32)
    for s in range(steps):
        for j in range(n_in):
            row = rank_ref[s : s + 1, j * region : (j + 1) * region]
            rk_ref[s * n_in + j : s * n_in + j + 1, :] = jnp.where(
                row < cnt_ref[s : s + 1, j : j + 1], row.astype(F32), big
            )
        row = orank_ref[s : s + 1, :]
        rk_ref[steps * n_in + s : steps * n_in + s + 1, :] = jnp.where(
            row < ocnt_ref[0:1, s : s + 1], row.astype(F32), big
        )
    old = lax.broadcasted_iota(jnp.int32, (region, region), 0)
    new = lax.broadcasted_iota(jnp.int32, (region, region), 1)
    shift = rpr.bit_length() - 1
    perm = jnp.where(old == (new & (rpr - 1)) * cpr + (new >> shift), 1.0, 0.0).astype(BF16)
    rp = jnp.dot(rk_ref[...].astype(BF16), perm, preferred_element_type=F32)
    rp_ref[...] = rp
    n_rk = rk_ref.shape[0]

    def eye(n):
        return jnp.where(
            lax.broadcasted_iota(jnp.int32, (n, LANES), 0) == lax.broadcasted_iota(jnp.int32, (n, LANES), 1), 1.0, 0.0
        ).astype(BF16)

    def turned(values):
        return lax.dot_general(
            values.astype(BF16), eye(values.shape[0]), (((0,), (0,)), ((), ())), preferred_element_type=F32
        ).astype(BF16)

    def spread(table, index, n):
        pick = jnp.where(lax.broadcasted_iota(jnp.int32, (LANES, n), 0) == index, 1.0, 0.0).astype(BF16)
        return jnp.dot(table, pick, preferred_element_type=F32)

    mt_ref[...] = turned(jnp.where(rp < big, 1.0, 0.0))
    for j in range(n_in):
        for s in range(steps):
            for h in range(halves):
                rsend[j, s * halves + h : s * halves + h + 1, :] = rp_ref[
                    s * n_in + j : s * n_in + j + 1, h * LANES : (h + 1) * LANES
                ]
    pl.semaphore_wait(barrier, n_in - 1 + n_out - 1)
    sends = []
    for d in range(1, n_in):
        copy = remote(rsend.at[inner(d)], rrecv.at[me], rs_sem.at[d], rr_sem.at[me], inner=inner(d))
        copy.start()
        sends.append(copy)

    order = []
    chunks = rows // LANES
    for a in range((chunks + 1) // 2):
        order.append(a)
        if chunks - 1 - a != a:
            order.append(chunks - 1 - a)

    def packet(s, j):
        return remote(send.at[s, j], recv.at[s, pl.ds(pl.multiple_of(me * slots, slots), slots)],
                      s_sem.at[s, j], r_sem.at[s, me], inner=j)

    slot_id = lax.broadcasted_iota(jnp.int32, (slots, region), 0).astype(F32)
    for s in range(steps):
        for copy in loads[s]:
            copy.wait()
        if s == 0:
            res_load.wait()
        for q in order:
            g = lax.dot_general(
                acts_v[s, :, q * LANES : (q + 1) * LANES], cot_v[s], (((0,), (0,)), ((), ())),
                preferred_element_type=F32,
            ) * scale
            for half in range(rpc):
                j = q * rpc + half
                chosen = spread(mt_ref[...], s * n_in + j, width)
                picks = jnp.where(rp_ref[s * n_in + j : s * n_in + j + 1, :] == slot_id, 1.0, 0.0).astype(BF16)
                parts = []
                for c in range(cpr):
                    where_at = pl.ds(region * j + c, rpr, stride=cpr)
                    acc = res_v[where_at, :] + g[half * rpr : (half + 1) * rpr, c * width : (c + 1) * width]
                    kept = jnp.where(chosen[c * rpr : (c + 1) * rpr] > 0.5, 0.0, acc)
                    (resid_ref if s == steps - 1 else res_v)[where_at, :] = kept
                    parts.append(acc)
                packed = jnp.dot(picks, jnp.concatenate(parts, axis=0).astype(BF16), preferred_element_type=F32)
                send[s, j] = packed.astype(BF16)

                @pl.when(me != j)
                def _():
                    packet(s, j).start()


    rrecv[me] = rsend[me]
    for d in range(1, n_in):
        i = inner(d)
        remote(rrecv.at[i], rrecv.at[i], rs_sem.at[d], rr_sem.at[i], inner=i).wait_recv()
    for i in range(n_in):
        for s in range(steps):
            for h in range(halves):
                rall_ref[s * n_in + i : s * n_in + i + 1, h * LANES : (h + 1) * LANES] = rrecv[
                    i, s * halves + h : s * halves + h + 1, :
                ]
    rt = turned(rall_ref[...])
    lane_id = lax.broadcasted_iota(jnp.int32, (region, slots), 1).astype(F32)
    for s in range(steps):
        for i in range(n_in):
            oh_ref[s, :, i * slots : (i + 1) * slots] = jnp.where(
                spread(rt, s * n_in + i, slots) == lane_id, 1.0, 0.0
            ).astype(BF16)

    oresid = jnp.concatenate([ores_ref[pl.ds(c, rpr, stride=cpr), :] for c in range(cpr)], axis=0)
    for s in range(steps):
        recv[s, pl.ds(pl.multiple_of(me * slots, slots), slots)] = send[s, me]
        for d in range(1, n_in):
            i = inner(d)
            spot = recv.at[s, pl.ds(pl.multiple_of(i * slots, slots), slots)]
            remote(spot, spot, s_sem.at[s, 0], r_sem.at[s, i], inner=i).wait_recv()
        oacc = jnp.dot(oh_ref[s], recv[s], preferred_element_type=F32) + oresid
        passed = spread(mt_ref[...], steps * n_in + s, width) > 0.5
        outgoing = jnp.where(passed, oacc, 0.0).astype(BF16)
        oresid = jnp.where(passed, 0.0, oacc)
        for c in range(n_out):
            xsend[s, c] = outgoing[c * rpr : (c + 1) * rpr]
        for d in range(1, n_out):
            copy = remote(xsend.at[s, outer(d)], xrecv.at[s, pod], xs_sem.at[s, d], xr_sem.at[s, pod], outer=outer(d))
            copy.start()
            sends.append(copy)
    for c in range(cpr):
        nores_ref[pl.ds(c, rpr, stride=cpr), :] = oresid[c * rpr : (c + 1) * rpr]

    total = jnp.zeros((rpr, width), F32)
    for s in range(steps):
        cross = xsend[s, pod].astype(F32)
        for d in range(1, n_out):
            i = outer(d)
            remote(xrecv.at[s, i], xrecv.at[s, i], xs_sem.at[s, d], xr_sem.at[s, i], outer=i).wait_recv()
            cross = cross + xrecv[s, i].astype(F32)
        total = total + cross.astype(BF16).astype(F32)
    ag[core, pod, z] = (-step_size * total).astype(BF16)

    def forward(zz, slot):
        piece = ag.at[core, pod, zz]
        for d in range(1, n_out):
            copy = remote(piece, piece, os_sem.at[slot, d], or_sem.at[pod, zz], outer=outer(d))
            copy.start()
            sends.append(copy)

    def hand_over(q, slot):
        piece = ag.at[core, q]
        copy = remote(piece, piece, ps_sem.at[slot], pr_sem.at[q], inner=partner)
        copy.start()
        sends.append(copy)

    own = ag.at[core, pod, z]
    for d in range(1, n_z):
        copy = remote(own, own, zs_sem.at[d], zr_sem.at[z], inner=inner(2 * d))
        copy.start()
        sends.append(copy)
    forward(z, 0)
    for d in range(1, n_z):
        zz = lax.rem(z + d, n_z)
        piece = ag.at[core, pod, zz]
        remote(piece, piece, zs_sem.at[d], zr_sem.at[zz], inner=inner(2 * d)).wait_recv()
        forward(zz, d)
    hand_over(pod, 0)
    for d in range(1, n_out):
        q = outer(d)
        for zz in range(n_z):
            piece = ag.at[core, q, zz]
            remote(piece, piece, os_sem.at[0, d], or_sem.at[q, zz], outer=q).wait_recv()
        hand_over(q, d)
    for d in range(n_out):
        q = outer(d)
        piece = ag.at[1 - core, q]
        remote(piece, piece, ps_sem.at[d], pr_sem.at[q], inner=partner).wait_recv()
    for zz in range(n_z):
        for k in range(2):
            j = zz * 2 + k
            for q in range(n_out):
                applied_ref[j * rpr : (j + 1) * rpr, q * width : (q + 1) * width] = ag[k, q, zz]

    for copy in sends:
        copy.wait_send()
    for s in range(steps):
        for j in range(n_in):

            @pl.when(me != j)
            def _():
                packet(s, j).wait_send()


def hand_out(*arrays):
    n = len(arrays)

    def kernel(*refs):
        sems = refs[2 * n]
        copies = [pltpu.make_async_copy(refs[k], refs[n + k], sems.at[k]) for k in range(n)]
        for copy in copies:
            copy.start()
        for copy in copies:
            copy.wait()

    return pl.pallas_call(
        kernel,
        out_shape=tuple(jax.ShapeDtypeStruct(a.shape, a.dtype) for a in arrays),
        in_specs=[pl.BlockSpec(memory_space=pltpu.VMEM)] * n,
        out_specs=tuple([pl.BlockSpec(memory_space=pltpu.HBM)] * n),
        scratch_shapes=[pltpu.SemaphoreType.DMA((n,))],
        compiler_params=pltpu.CompilerParams(vmem_limit_bytes=4 << 20),
    )(*arrays)


def fits(owners, pods, steps, rows, cols, blocks, width, region, slots):
    if width != LANES or slots % LANES or region % LANES or region > 256 or cols % width:
        return False
    cpr = cols // width
    rpr = region // cpr
    return (
        cpr == pods and cpr * rpr == region and rpr % 16 == 0 and LANES % rpr == 0 and rpr & (rpr - 1) == 0
        and rows % LANES == 0 and owners >= 4 and owners % 2 == 0
        and rpr * owners == rows and steps * (owners + 1) <= LANES and steps * (region // LANES) <= 8
    )


def per_device_fused(acts, cotangent, residual, owner_residual, in_count, in_rank, out_count, out_rank):
    n_in = lax.axis_size("inner")
    n_out = lax.axis_size("outer")
    steps, tokens, rows = acts.shape[1:]
    cols = cotangent.shape[3]
    blocks, width = residual.shape[1:]
    region = blocks // n_in
    slots = max(1, region // 2)
    if not fits(n_in, n_out, steps, rows, cols, blocks, width, region, slots):
        return per_device(acts, cotangent, residual, owner_residual, in_count, in_rank, out_count, out_rank)
    scale = 1.0 / math.sqrt(tokens * n_in)
    rpr = region // n_out
    n_z = n_in // 2
    n_rk = -(-steps * (n_in + 1) // 16) * 16
    n_ra = -(-steps * n_in // 16) * 16
    vmem = pl.BlockSpec(memory_space=pltpu.VMEM)
    anywhere = pl.BlockSpec(memory_space=pltpu.HBM)
    dma = pltpu.SemaphoreType.DMA
    applied, resid, oresid = pl.pallas_call(
        functools.partial(fused_kernel, (n_in, n_out, steps, scale, region, slots, width)),
        out_shape=(
            jax.ShapeDtypeStruct((rows, cols), BF16),
            jax.ShapeDtypeStruct((blocks, width), F32),
            jax.ShapeDtypeStruct((region, width), F32),
        ),
        in_specs=[anywhere, anywhere, anywhere, vmem, vmem, vmem, vmem, vmem],
        out_specs=(vmem, vmem, vmem),
        scratch_shapes=[
            pltpu.VMEM((steps, tokens, rows), BF16),
            pltpu.VMEM((steps, tokens, cols), BF16),
            pltpu.VMEM((blocks, width), F32),
            pltpu.VMEM((n_rk, region), F32),
            pltpu.VMEM((n_rk, region), F32),
            pltpu.VMEM((region, LANES), BF16),
            pltpu.VMEM((n_in, 8, LANES), F32),
            pltpu.VMEM((n_in, 8, LANES), F32),
            pltpu.VMEM((n_ra, region), F32),
            pltpu.VMEM((steps, region, n_in * slots), BF16),
            pltpu.VMEM((steps, n_in, slots, width), BF16),
            pltpu.VMEM((steps, n_in * slots, width), BF16),
            pltpu.VMEM((steps, n_out, rpr, width), BF16),
            pltpu.VMEM((steps, n_out, rpr, width), BF16),
            pltpu.VMEM((2, n_out, n_z, rpr, width), BF16),
            dma((2 * steps + 1,)),
            dma((n_in,)),
            dma((n_in,)),
            dma((steps, n_in)),
            dma((steps, n_in)),
            dma((steps, n_out)),
            dma((steps, n_out)),
            dma((n_z,)),
            dma((n_z,)),
            dma((n_z, n_out)),
            dma((n_out, n_z)),
            dma((n_out,)),
            dma((n_out,)),
        ],
        compiler_params=pltpu.CompilerParams(collective_id=0, has_side_effects=True, vmem_limit_bytes=24 << 20),
    )(acts[0], cotangent[0], residual[0], owner_residual[0], in_count[0], in_rank[0], out_count, out_rank[0])
    applied, resid, oresid = hand_out(applied, resid, oresid)
    return applied, resid[None], oresid[None]


def solution(mesh):
    return jax.shard_map(
        per_device_fused,
        mesh=mesh,
        in_specs=(
            P(("outer", "inner"), None, None, None),
            P(("outer", "inner"), None, None, None),
            P(("outer", "inner"), None, None),
            P(("outer", "inner"), None, None),
            P(("outer", "inner"), None, None),
            P(("outer", "inner"), None, None),
            P(("outer", "inner"), None),
            P(("outer", "inner"), None, None),
        ),
        out_specs=(P(), P(("outer", "inner"), None, None), P(("outer", "inner"), None, None)),
        check_vma=False,
    )
```

```python
import functools
import math

import jax
import jax.numpy as jnp
from jax import lax
from jax.experimental import pallas as pl
from jax.experimental.pallas import tpu as pltpu
from jax.sharding import PartitionSpec as P

step_size = 0.0625


def select_blocks(resid, grad, ranks_flat, counts, owners, region, width):
    blocks = resid.shape[0]
    accum = (resid + grad.reshape(blocks, width)).reshape(owners, region, width)
    ranks = ranks_flat.reshape(owners, region)
    chosen = (ranks < counts[:, None])[..., None]
    new_resid = jnp.where(chosen, jnp.float32(0.0), accum).reshape(blocks, width)
    return (accum, ranks, chosen, new_resid)


def pack_slots(accum, ranks, counts, slots, region):
    order = lax.iota(jnp.int32, slots)
    picks = (ranks[:, None, :] == order[None, :, None]) & (
        order[None, :, None] < counts[:, None, None]
    )
    picks_f = picks.astype(jnp.float32)
    places = lax.iota(jnp.int32, region).astype(jnp.float32)
    packed = jnp.einsum("nkr,nrd->nkd", picks_f, accum, precision=lax.Precision.HIGHEST)
    where_at = jnp.einsum("nkr,r->nk", picks_f, places, precision=lax.Precision.HIGHEST)
    return (packed, where_at)


def unpack_slots(arrived, spots, region, width):
    places = lax.iota(jnp.int32, region).astype(jnp.float32)
    placed = (spots.reshape(-1)[:, None] == places[None, :]).astype(jnp.float32)
    return jnp.einsum(
        "mr,md->rd", placed, arrived.reshape(-1, width), precision=lax.Precision.HIGHEST
    )


def owner_section(pod_sum, oresid, ranks_out, count_out):
    owner_acc = pod_sum + oresid
    passed = (ranks_out < count_out)[:, None]
    outgoing = jnp.where(passed, owner_acc, jnp.float32(0.0))
    kept = jnp.where(passed, jnp.float32(0.0), owner_acc)
    return (outgoing, kept)


def per_device(acts, cotangent, residual, owner_residual, in_count, in_rank, out_count, out_rank):
    owners = lax.axis_size("inner")
    steps = acts.shape[1]
    tokens = acts.shape[2]
    rows = acts.shape[3]
    cols = cotangent.shape[3]
    blocks = residual.shape[1]
    width = residual.shape[2]
    region = blocks // owners
    slots = max(1, region // 2)
    scale = 1.0 / math.sqrt(tokens * owners)
    resid = residual[0]
    oresid = owner_residual[0]
    crosses = []
    packs = []
    spots_all = []
    for step in range(steps):
        grad = (
            jnp.einsum(
                "tr,tc->rc", acts[0, step], cotangent[0, step], preferred_element_type=jnp.float32
            )
            * scale
        )
        counts = in_count[0, step]
        accum, ranks, chosen, resid = select_blocks(
            resid, grad, in_rank[0, step], counts, owners, region, width
        )
        packed, where_at = pack_slots(accum, ranks, counts, slots, region)
        packs.append(packed)
        spots_all.append(where_at)
    arrived, spots = (
        lax.all_to_all(
            jnp.concatenate(packs, axis=1), "inner", split_axis=0, concat_axis=0, tiled=True
        ),
        lax.all_to_all(
            jnp.concatenate(spots_all, axis=1), "inner", split_axis=0, concat_axis=0, tiled=True
        ),
    )
    outgoings = []
    for step in range(steps):
        pod_sum = unpack_slots(
            arrived[:, step * slots : (step + 1) * slots],
            spots[:, step * slots : (step + 1) * slots],
            region,
            width,
        )
        outgoing, oresid = owner_section(pod_sum, oresid, out_rank[0, step], out_count[0, step])
        outgoings.append(outgoing)
    summed = lax.psum(jnp.stack(outgoings), "outer")
    for step in range(steps):
        crosses.append(summed[step])
    deltas = []
    for cross in crosses:
        delta = cross.astype(jnp.bfloat16)
        deltas.append(lax.all_gather(delta, "inner", axis=0, tiled=True))
    total = deltas[0].astype(jnp.float32)
    for later in deltas[1:]:
        total = total + later.astype(jnp.float32)
    applied = (-step_size * total).astype(jnp.bfloat16)
    return (applied.reshape(rows, cols), resid[None], oresid[None])


LANES = 128
F32 = jnp.float32
BF16 = jnp.bfloat16


def fused_kernel(
    dims,
    acts_hbm, cot_hbm, res_hbm, ores_hbm, cnt_hbm, rank_hbm, ocnt_hbm, orank_hbm,
    applied_ref, resid_ref, nores_ref,
    ores_ref, cnt_ref, rank_ref, ocnt_ref, orank_ref, small_sem,
    acts_v, cot_v, res_v, rk_ref, rp_ref, mt_ref, rsend, rrecv, rall_ref, oh_ref,
    send, recv, xsend, xrecv, ag,
    in_sem, rs_sem, rr_sem, s_sem, r_sem, xs_sem, xr_sem,
    zs_sem, zr_sem, os_sem, or_sem, ps_sem, pr_sem,
):
    n_in, n_out, steps, scale, region, slots, width = dims
    rows, cols = acts_v.shape[2], cot_v.shape[2]
    cpr = cols // width
    rpr = region // cpr
    halves = region // LANES
    rpc = LANES // rpr
    n_z = n_in // 2
    big = float(region)
    me = lax.axis_index("inner")
    pod = lax.axis_index("outer")
    core = lax.rem(me, 2)
    z = lax.div(me, 2)
    partner = me + 1 - 2 * core

    def inner(d):
        return lax.rem(me + d, n_in)

    def outer(d):
        return lax.rem(pod + d, n_out)

    def remote(src, dst, ssem, rsem, **device):
        return pltpu.make_async_remote_copy(
            src_ref=src, dst_ref=dst, send_sem=ssem, recv_sem=rsem,
            device_id=device, device_id_type=pl.DeviceIdType.MESH,
        )

    small = [
        pltpu.make_async_copy(src, dst, small_sem.at[k])
        for k, (src, dst) in enumerate(
            ((rank_hbm, rank_ref), (cnt_hbm, cnt_ref), (orank_hbm, orank_ref), (ocnt_hbm, ocnt_ref), (ores_hbm, ores_ref))
        )
    ]
    for copy in small:
        copy.start()
    loads = []
    for s in range(steps):
        pair = [
            pltpu.make_async_copy(acts_hbm.at[s], acts_v.at[s], in_sem.at[2 * s]),
            pltpu.make_async_copy(cot_hbm.at[s], cot_v.at[s], in_sem.at[2 * s + 1]),
        ]
        for copy in pair:
            copy.start()
        loads.append(pair)
        if s == 0:
            res_load = pltpu.make_async_copy(res_hbm, res_v, in_sem.at[2 * steps])
            res_load.start()

    barrier = pltpu.get_barrier_semaphore()
    for d in range(1, n_in):
        pl.semaphore_signal(barrier, inc=1, device_id={"inner": inner(d)}, device_id_type=pl.DeviceIdType.MESH)
    for d in range(1, n_out):
        pl.semaphore_signal(barrier, inc=1, device_id={"outer": outer(d)}, device_id_type=pl.DeviceIdType.MESH)

    rk_ref[...] = jnp.full(rk_ref.shape, big, F32)
    for copy in small:
        copy.wait()
    for s in range(steps):
        for j in range(n_in):
            row = rank_ref[s : s + 1, j * region : (j + 1) * region]
            rk_ref[s * n_in + j : s * n_in + j + 1, :] = jnp.where(
                row < cnt_ref[s : s + 1, j : j + 1], row.astype(F32), big
            )
        row = orank_ref[s : s + 1, :]
        rk_ref[steps * n_in + s : steps * n_in + s + 1, :] = jnp.where(
            row < ocnt_ref[0:1, s : s + 1], row.astype(F32), big
        )
    old = lax.broadcasted_iota(jnp.int32, (region, region), 0)
    new = lax.broadcasted_iota(jnp.int32, (region, region), 1)
    shift = rpr.bit_length() - 1
    perm = jnp.where(old == (new & (rpr - 1)) * cpr + (new >> shift), 1.0, 0.0).astype(BF16)
    rp = jnp.dot(rk_ref[...].astype(BF16), perm, preferred_element_type=F32)
    rp_ref[...] = rp
    n_rk = rk_ref.shape[0]

    def eye(n):
        return jnp.where(
            lax.broadcasted_iota(jnp.int32, (n, LANES), 0) == lax.broadcasted_iota(jnp.int32, (n, LANES), 1), 1.0, 0.0
        ).astype(BF16)

    def turned(values):
        return lax.dot_general(
            values.astype(BF16), eye(values.shape[0]), (((0,), (0,)), ((), ())), preferred_element_type=F32
        ).astype(BF16)

    def spread(table, index, n):
        pick = jnp.where(lax.broadcasted_iota(jnp.int32, (LANES, n), 0) == index, 1.0, 0.0).astype(BF16)
        return jnp.dot(table, pick, preferred_element_type=F32)

    mt_ref[...] = turned(jnp.where(rp < big, 1.0, 0.0))
    for j in range(n_in):
        for s in range(steps):
            for h in range(halves):
                rsend[j, s * halves + h : s * halves + h + 1, :] = rp_ref[
                    s * n_in + j : s * n_in + j + 1, h * LANES : (h + 1) * LANES
                ]
    pl.semaphore_wait(barrier, n_in - 1 + n_out - 1)
    sends = []
    for d in range(1, n_in):
        copy = remote(rsend.at[inner(d)], rrecv.at[me], rs_sem.at[d], rr_sem.at[me], inner=inner(d))
        copy.start()
        sends.append(copy)

    order = []
    chunks = rows // LANES
    for a in range((chunks + 1) // 2):
        order.append(a)
        if chunks - 1 - a != a:
            order.append(chunks - 1 - a)

    def packet(s, j):
        return remote(send.at[s, j], recv.at[s, pl.ds(pl.multiple_of(me * slots, slots), slots)],
                      s_sem.at[s, j], r_sem.at[s, me], inner=j)

    slot_id = lax.broadcasted_iota(jnp.int32, (slots, region), 0).astype(F32)
    for s in range(steps):
        for copy in loads[s]:
            copy.wait()
        if s == 0:
            res_load.wait()
        for q in order:
            g = lax.dot_general(
                acts_v[s, :, q * LANES : (q + 1) * LANES], cot_v[s], (((0,), (0,)), ((), ())),
                preferred_element_type=F32,
            ) * scale
            for half in range(rpc):
                j = q * rpc + half
                chosen = spread(mt_ref[...], s * n_in + j, width)
                picks = jnp.where(rp_ref[s * n_in + j : s * n_in + j + 1, :] == slot_id, 1.0, 0.0).astype(BF16)
                parts = []
                for c in range(cpr):
                    where_at = pl.ds(region * j + c, rpr, stride=cpr)
                    acc = res_v[where_at, :] + g[half * rpr : (half + 1) * rpr, c * width : (c + 1) * width]
                    kept = jnp.where(chosen[c * rpr : (c + 1) * rpr] > 0.5, 0.0, acc)
                    (resid_ref if s == steps - 1 else res_v)[where_at, :] = kept
                    parts.append(acc)
                packed = jnp.dot(picks, jnp.concatenate(parts, axis=0).astype(BF16), preferred_element_type=F32)
                send[s, j] = packed.astype(BF16)

                @pl.when(me != j)
                def _():
                    packet(s, j).start()


    rrecv[me] = rsend[me]
    for d in range(1, n_in):
        i = inner(d)
        remote(rrecv.at[i], rrecv.at[i], rs_sem.at[d], rr_sem.at[i], inner=i).wait_recv()
    for i in range(n_in):
        for s in range(steps):
            for h in range(halves):
                rall_ref[s * n_in + i : s * n_in + i + 1, h * LANES : (h + 1) * LANES] = rrecv[
                    i, s * halves + h : s * halves + h + 1, :
                ]
    rt = turned(rall_ref[...])
    lane_id = lax.broadcasted_iota(jnp.int32, (region, slots), 1).astype(F32)
    for s in range(steps):
        for i in range(n_in):
            oh_ref[s, :, i * slots : (i + 1) * slots] = jnp.where(
                spread(rt, s * n_in + i, slots) == lane_id, 1.0, 0.0
            ).astype(BF16)

    oresid = jnp.concatenate([ores_ref[pl.ds(c, rpr, stride=cpr), :] for c in range(cpr)], axis=0)
    for s in range(steps):
        recv[s, pl.ds(pl.multiple_of(me * slots, slots), slots)] = send[s, me]
        for d in range(1, n_in):
            i = inner(d)
            spot = recv.at[s, pl.ds(pl.multiple_of(i * slots, slots), slots)]
            remote(spot, spot, s_sem.at[s, 0], r_sem.at[s, i], inner=i).wait_recv()
        oacc = jnp.dot(oh_ref[s], recv[s], preferred_element_type=F32) + oresid
        passed = spread(mt_ref[...], steps * n_in + s, width) > 0.5
        outgoing = jnp.where(passed, oacc, 0.0).astype(BF16)
        oresid = jnp.where(passed, 0.0, oacc)
        for c in range(n_out):
            xsend[s, c] = outgoing[c * rpr : (c + 1) * rpr]
        for d in range(1, n_out):
            copy = remote(xsend.at[s, outer(d)], xrecv.at[s, pod], xs_sem.at[s, d], xr_sem.at[s, pod], outer=outer(d))
            copy.start()
            sends.append(copy)
    for c in range(cpr):
        nores_ref[pl.ds(c, rpr, stride=cpr), :] = oresid[c * rpr : (c + 1) * rpr]

    total = jnp.zeros((rpr, width), F32)
    for s in range(steps):
        cross = xsend[s, pod].astype(F32)
        for d in range(1, n_out):
            i = outer(d)
            remote(xrecv.at[s, i], xrecv.at[s, i], xs_sem.at[s, d], xr_sem.at[s, i], outer=i).wait_recv()
            cross = cross + xrecv[s, i].astype(F32)
        total = total + cross.astype(BF16).astype(F32)
    ag[core, pod, z] = (-step_size * total).astype(BF16)

    def forward(zz, slot):
        piece = ag.at[core, pod, zz]
        for d in range(1, n_out):
            copy = remote(piece, piece, os_sem.at[slot, d], or_sem.at[pod, zz], outer=outer(d))
            copy.start()
            sends.append(copy)

    def hand_over(q, slot):
        piece = ag.at[core, q]
        copy = remote(piece, piece, ps_sem.at[slot], pr_sem.at[q], inner=partner)
        copy.start()
        sends.append(copy)

    own = ag.at[core, pod, z]
    for d in range(1, n_z):
        copy = remote(own, own, zs_sem.at[d], zr_sem.at[z], inner=inner(2 * d))
        copy.start()
        sends.append(copy)
    forward(z, 0)
    for d in range(1, n_z):
        zz = lax.rem(z + d, n_z)
        piece = ag.at[core, pod, zz]
        remote(piece, piece, zs_sem.at[d], zr_sem.at[zz], inner=inner(2 * d)).wait_recv()
        forward(zz, d)
    hand_over(pod, 0)
    for d in range(1, n_out):
        q = outer(d)
        for zz in range(n_z):
            piece = ag.at[core, q, zz]
            remote(piece, piece, os_sem.at[0, d], or_sem.at[q, zz], outer=q).wait_recv()
        hand_over(q, d)
    for d in range(n_out):
        q = outer(d)
        piece = ag.at[1 - core, q]
        remote(piece, piece, ps_sem.at[d], pr_sem.at[q], inner=partner).wait_recv()
    for zz in range(n_z):
        for k in range(2):
            j = zz * 2 + k
            for q in range(n_out):
                applied_ref[j * rpr : (j + 1) * rpr, q * width : (q + 1) * width] = ag[k, q, zz]

    for copy in sends:
        copy.wait_send()
    for s in range(steps):
        for j in range(n_in):

            @pl.when(me != j)
            def _():
                packet(s, j).wait_send()


def hand_out(*arrays):
    n = len(arrays)

    def kernel(*refs):
        sems = refs[2 * n]
        copies = [pltpu.make_async_copy(refs[k], refs[n + k], sems.at[k]) for k in range(n)]
        for copy in copies:
            copy.start()
        for copy in copies:
            copy.wait()

    return pl.pallas_call(
        kernel,
        out_shape=tuple(jax.ShapeDtypeStruct(a.shape, a.dtype) for a in arrays),
        in_specs=[pl.BlockSpec(memory_space=pltpu.VMEM)] * n,
        out_specs=tuple([pl.BlockSpec(memory_space=pltpu.HBM)] * n),
        scratch_shapes=[pltpu.SemaphoreType.DMA((n,))],
        compiler_params=pltpu.CompilerParams(vmem_limit_bytes=4 << 20),
    )(*arrays)


def fits(owners, pods, steps, rows, cols, blocks, width, region, slots):
    if width != LANES or slots % LANES or region % LANES or region > 256 or cols % width:
        return False
    cpr = cols // width
    rpr = region // cpr
    return (
        cpr == pods and cpr * rpr == region and rpr % 16 == 0 and LANES % rpr == 0 and rpr & (rpr - 1) == 0
        and rows % LANES == 0 and owners >= 4 and owners % 2 == 0
        and rpr * owners == rows and steps * (owners + 1) <= LANES and steps * (region // LANES) <= 8
    )


def per_device_fused(acts, cotangent, residual, owner_residual, in_count, in_rank, out_count, out_rank):
    n_in = lax.axis_size("inner")
    n_out = lax.axis_size("outer")
    steps, tokens, rows = acts.shape[1:]
    cols = cotangent.shape[3]
    blocks, width = residual.shape[1:]
    region = blocks // n_in
    slots = max(1, region // 2)
    if not fits(n_in, n_out, steps, rows, cols, blocks, width, region, slots):
        return per_device(acts, cotangent, residual, owner_residual, in_count, in_rank, out_count, out_rank)
    scale = 1.0 / math.sqrt(tokens * n_in)
    rpr = region // n_out
    n_z = n_in // 2
    n_rk = -(-steps * (n_in + 1) // 16) * 16
    n_ra = -(-steps * n_in // 16) * 16
    vmem = pl.BlockSpec(memory_space=pltpu.VMEM)
    anywhere = pl.BlockSpec(memory_space=pltpu.HBM)
    dma = pltpu.SemaphoreType.DMA
    applied, resid, oresid = pl.pallas_call(
        functools.partial(fused_kernel, (n_in, n_out, steps, scale, region, slots, width)),
        out_shape=(
            jax.ShapeDtypeStruct((rows, cols), BF16),
            jax.ShapeDtypeStruct((blocks, width), F32),
            jax.ShapeDtypeStruct((region, width), F32),
        ),
        in_specs=[anywhere] * 8,
        out_specs=(vmem, vmem, vmem),
        scratch_shapes=[
            pltpu.VMEM((region, width), F32),
            pltpu.VMEM((steps, n_in), jnp.int32),
            pltpu.VMEM((steps, blocks), jnp.int32),
            pltpu.VMEM((1, steps), jnp.int32),
            pltpu.VMEM((steps, region), jnp.int32),
            dma((5,)),
            pltpu.VMEM((steps, tokens, rows), BF16),
            pltpu.VMEM((steps, tokens, cols), BF16),
            pltpu.VMEM((blocks, width), F32),
            pltpu.VMEM((n_rk, region), F32),
            pltpu.VMEM((n_rk, region), F32),
            pltpu.VMEM((region, LANES), BF16),
            pltpu.VMEM((n_in, 8, LANES), F32),
            pltpu.VMEM((n_in, 8, LANES), F32),
            pltpu.VMEM((n_ra, region), F32),
            pltpu.VMEM((steps, region, n_in * slots), BF16),
            pltpu.VMEM((steps, n_in, slots, width), BF16),
            pltpu.VMEM((steps, n_in * slots, width), BF16),
            pltpu.VMEM((steps, n_out, rpr, width), BF16),
            pltpu.VMEM((steps, n_out, rpr, width), BF16),
            pltpu.VMEM((2, n_out, n_z, rpr, width), BF16),
            dma((2 * steps + 1,)),
            dma((n_in,)),
            dma((n_in,)),
            dma((steps, n_in)),
            dma((steps, n_in)),
            dma((steps, n_out)),
            dma((steps, n_out)),
            dma((n_z,)),
            dma((n_z,)),
            dma((n_z, n_out)),
            dma((n_out, n_z)),
            dma((n_out,)),
            dma((n_out,)),
        ],
        compiler_params=pltpu.CompilerParams(collective_id=0, has_side_effects=True, vmem_limit_bytes=48 << 20),
    )(*(
        pltpu.with_memory_space_constraint(a, pltpu.HBM)
        for a in (
            acts[0], cotangent[0], residual[0], owner_residual[0], in_count[0], in_rank[0], out_count, out_rank[0]
        )
    ))
    applied, resid, oresid = hand_out(applied, resid, oresid)
    return applied, resid[None], oresid[None]


def solution(mesh):
    return jax.shard_map(
        per_device_fused,
        mesh=mesh,
        in_specs=(
            P(("outer", "inner"), None, None, None),
            P(("outer", "inner"), None, None, None),
            P(("outer", "inner"), None, None),
            P(("outer", "inner"), None, None),
            P(("outer", "inner"), None, None),
            P(("outer", "inner"), None, None),
            P(("outer", "inner"), None),
            P(("outer", "inner"), None, None),
        ),
        out_specs=(P(), P(("outer", "inner"), None, None), P(("outer", "inner"), None, None)),
        check_vma=False,
    )
```
